32 devices in a mesh: pb: 2 (over core), row: 4 (over y, x), col: 4 (over z).
Axes of the slice: x: 2, y: 2, z: 4, core: 2. Of those that a mesh axis runs over, the one named last changes fastest.
Arguments:
- chol: bfloat16 [64, 1344, 1344], P('pb', 'row', 'col'), may hold values from -0.29882812 to 0.29882812
- amplitudes: bfloat16 [144, 1200], P(None, 'row'), may hold values from -0.59765625 to 0.59765625
Outputs:
- dressed: bfloat16 [64, 1344, 1344], P(('pb', 'row', 'col'))
- fock: float32 [1344, 1344], P('row', 'col')
The draws below stay inside these ranges and needn't reach their ends.
All inputs are finite; a program needn't handle non-finite values.
Results may differ from the reference program's by a relative error of at most 0.02.
Values may be sent and summed in bfloat16 or wider, within the bound.
A program may use at most 128 MiB of HBM per device.

```python
import jax
import jax.numpy as jnp
from jax import lax

NG = 16
OCC = 144
VIR = 1200
OG = 9
VG = 75
SH = 84
NORB = 1344
Q = 64
N_ROW = 4


def levels(rng, dims, cuts, smallest, high):
    def one(dim, shards_of):
        steps = jax.random.uniform(jax.random.fold_in(jax.random.fold_in(rng, 6), dim), (shards_of,), jnp.float32, smallest / len(cuts), high / len(cuts))
        return jnp.repeat(jnp.exp(steps), dims[dim] // shards_of).reshape((-1,) + (1,) * (len(dims) - dim - 1))

    gain = one(*cuts[0])
    for cut in cuts[1:]:
        gain = gain * one(*cut)
    return gain


def normal_values(own_key, extent, scale, most, shards=(), held_as=jnp.bfloat16):
    values = scale * jax.random.normal(own_key, extent, jnp.float32)
    if shards:
        values = values * levels(own_key, extent, shards, -0.22, 0.18)
    return jnp.clip(values, -most, most).astype(held_as)


def setup_inputs(seed: int = 0) -> dict:
    splits = jax.random.split(jax.random.key(seed), 3)
    return {
        "chol": normal_values(splits[0], (Q, NORB, NORB), 0.05, 0.29882812, ((0, 2), (1, 4), (2, 4))),
        "amplitudes": normal_values(splits[1], (OCC, VIR), 0.1, 0.59765625, ((1, 4),)),
    }


block_vectors = 16


def reference(chol, amplitudes):
    amp_float = amplitudes.astype(jnp.float32)
    span = (NG // N_ROW) * VG
    amp_blocks = jnp.moveaxis(amp_float.reshape(OCC, N_ROW, span), 1, 0)

    def one_block(total, piece):
        layered = piece.reshape(block_vectors, NG, SH, NORB)
        occ_rows = layered[:, :, :OG, :].astype(jnp.float32)
        vir_rows = layered[:, :, OG:, :].astype(jnp.float32).reshape(block_vectors, N_ROW, span, NORB)
        vir_blocks = jnp.moveaxis(vir_rows, 1, 0)

        def add_block(acc, pair):
            amp_part, rows_part = pair
            term = jnp.einsum("ia,qab->qib", amp_part, rows_part)
            term = lax.optimization_barrier(term.astype(jnp.bfloat16))
            return acc + term.astype(jnp.float32), None

        shift, unused = lax.scan(add_block, jnp.zeros((block_vectors, OCC, NORB), jnp.float32), (amp_blocks, vir_blocks))
        occ_new = occ_rows - shift.reshape(block_vectors, NG, OG, NORB)
        primed = jnp.concatenate([occ_new, layered[:, :, OG:, :].astype(jnp.float32)], axis=2)
        primed = primed.reshape(block_vectors, NORB, NORB).astype(jnp.bfloat16)
        columns = primed.reshape(block_vectors, NORB, NG, SH).astype(jnp.float32)
        occ_cols = columns[..., :OG].reshape(block_vectors, NORB, OCC)
        extra = jnp.einsum("qpi,ia->qpa", occ_cols, amp_float).reshape(block_vectors, NORB, NG, VG)
        dressed = jnp.concatenate([columns[..., :OG], columns[..., OG:] + extra], axis=3)
        dressed = dressed.reshape(block_vectors, NORB, NORB).astype(jnp.bfloat16)
        dense = dressed.astype(jnp.float32)
        diagonal = jnp.diagonal(dense, axis1=1, axis2=2).reshape(block_vectors, NG, SH)[:, :, :OG]
        weight = jnp.sum(diagonal, axis=(1, 2))
        dcols = dense.reshape(block_vectors, NORB, NG, SH)[..., :OG].reshape(block_vectors, NORB, OCC)
        drows = dense.reshape(block_vectors, NG, SH, NORB)[:, :, :OG, :].reshape(block_vectors, OCC, NORB)
        coulomb = jnp.einsum("q,qab->ab", weight, dense)
        swapped = jnp.einsum("qpi,qib->pb", dcols, drows)
        return total + 2.0 * coulomb - swapped, dressed

    stacked = chol.reshape(Q // block_vectors, block_vectors, NORB, NORB)
    fock, dressed = lax.scan(one_block, jnp.zeros((NORB, NORB), jnp.float32), stacked)
    return dressed.reshape(Q, NORB, NORB), fock
```

```python
import functools
import jax
import jax.numpy as jnp
from jax import lax
from jax.experimental import pallas as pl
from jax.experimental.pallas import tpu as pltpu
from jax.sharding import PartitionSpec as P

OG = 9
VG = 75
SH = 84
MESH = pl.DeviceIdType.MESH


def exchange_kernel(R, C, chol, amp, recv, amp_all, own, send_sem, recv_sem, asend, arecv, lsem):
    r = lax.axis_index("row")
    c = lax.axis_index("col")
    nq = recv.shape[1]
    me = r * C + c
    mine = pltpu.make_async_copy(chol.at[pl.ds(me * nq, nq)], own, lsem.at[0])
    mine.start()
    amp_mine = pltpu.make_async_copy(amp, amp_all.at[r], lsem.at[2])
    amp_mine.start()
    peers = [(dr, dc) for dr in range(R) for dc in range(C) if (dr, dc) != (0, 0)]
    peers.sort(key=lambda t: -min(t[1], C - t[1]))
    barrier = pltpu.get_barrier_semaphore()
    for dr, dc in peers:
        pl.semaphore_signal(
            barrier, inc=1, device_id={"row": lax.rem(r + dr, R), "col": lax.rem(c + dc, C)}, device_id_type=MESH
        )
    pl.semaphore_wait(barrier, len(peers))
    copies = []
    for dr in range(1, R):
        copies.append(
            pltpu.make_async_remote_copy(
                src_ref=amp,
                dst_ref=amp_all.at[r],
                send_sem=asend.at[dr],
                recv_sem=arecv.at[dr],
                device_id={"row": lax.rem(r + dr, R), "col": c},
                device_id_type=MESH,
            )
        )
        copies[-1].start()
    for dr, dc in peers:
        tr = lax.rem(r + dr, R)
        tc = lax.rem(c + dc, C)
        k = dr * C + dc
        copies.append(
            pltpu.make_async_remote_copy(
                src_ref=chol.at[pl.ds((tr * C + tc) * nq, nq)],
                dst_ref=recv.at[me],
                send_sem=send_sem.at[k],
                recv_sem=recv_sem.at[k],
                device_id={"row": tr, "col": tc},
                device_id_type=MESH,
            )
        )
        copies[-1].start()
    mine.wait()
    out = pltpu.make_async_copy(own, recv.at[me], lsem.at[1])
    out.start()
    amp_mine.wait()
    out.wait()
    for copy in copies:
        copy.wait()


def dress_kernel(R, C, n, recv, amps, pick, pick_t, dressed, fock, primed, cols, total):
    q = pl.program_id(0)
    th = cw = recv.shape[3]
    for j in range(C):
        shift = None
        tiles = []
        for i in range(C):
            if n == 1:
                tile = recv[i * C + j, 0]
            else:
                tile = jnp.concatenate(
                    [recv[(i * n + m) * C + j, 0].astype(jnp.float32) for m in range(n)], axis=0
                ).astype(jnp.bfloat16)
            tiles.append(tile)
            term = jnp.dot(amps[i], tile, preferred_element_type=jnp.float32)
            term = term.astype(jnp.bfloat16).astype(jnp.float32)
            shift = term if shift is None else shift + term
        hi = shift.astype(jnp.bfloat16)
        lo = (shift - hi.astype(jnp.float32)).astype(jnp.bfloat16)
        for i in range(C):
            placed = jnp.dot(pick[i], hi, preferred_element_type=jnp.float32)
            placed = placed + jnp.dot(pick[i], lo, preferred_element_type=jnp.float32)
            primed[i, j] = (tiles[i].astype(jnp.float32) - placed).astype(jnp.bfloat16)
    weight = jnp.zeros((1, 1), jnp.float32)
    for i in range(C):
        occ = None
        for j in range(C):
            part = jnp.dot(primed[i, j], pick[j], preferred_element_type=jnp.float32)
            occ = part if occ is None else occ + part
        cols[i] = occ.astype(jnp.bfloat16)
        diag = occ * pick[i].astype(jnp.float32)
        weight = weight + jnp.sum(jnp.sum(diag, axis=1, keepdims=True), axis=0, keepdims=True)
    for i in range(C):
        strip = []
        for j in range(C):
            extra = jnp.dot(cols[i], amps[j], preferred_element_type=jnp.float32)
            tile = (primed[i, j].astype(jnp.float32) + extra).astype(jnp.bfloat16)
            primed[i, j] = tile
            strip.append(tile.astype(jnp.float32))
        dressed[0, pl.ds(i * th, th), :] = jnp.concatenate(strip, axis=1).astype(jnp.bfloat16)
    for j in range(C):
        rows = None
        for i in range(C):
            part = jnp.dot(pick_t[i], primed[i, j], preferred_element_type=jnp.float32)
            rows = part if rows is None else rows + part
        rows = rows.astype(jnp.bfloat16)
        for i in range(C):
            swapped = jnp.dot(cols[i], rows, preferred_element_type=jnp.float32)
            value = 2.0 * weight * primed[i, j].astype(jnp.float32) - swapped

            @pl.when(q == 0)
            def _():
                total[i, j] = value

            @pl.when(q > 0)
            def _():
                total[i, j] = total[i, j] + value

            @pl.when(q == pl.num_programs(0) - 1)
            def _():
                fock[j, i] = total[i, j].astype(jnp.bfloat16)


def reduce_kernel(B, R, C, part, out, got1, half, got2, block, got3, s1, r1, s2, r2, s3, r3, s4, r4):
    b = lax.axis_index("pb")
    r = lax.axis_index("row")
    c = lax.axis_index("col")
    share = C // B
    barrier = pltpu.get_barrier_semaphore()
    for axis, index, size in (("pb", b, B), ("row", r, R), ("col", c, C)):
        for d in range(1, size):
            pl.semaphore_signal(barrier, inc=1, device_id={axis: lax.rem(index + d, size)}, device_id_type=MESH)
    pl.semaphore_wait(barrier, B + R + C - 3)

    copies = []
    for d in range(1, B):
        to = lax.rem(b + d, B)
        copies.append(
            pltpu.make_async_remote_copy(
                src_ref=part.at[to], dst_ref=got1.at[d - 1], send_sem=s1.at[d], recv_sem=r1.at[d],
                device_id={"pb": to}, device_id_type=MESH,
            )
        )
        copies[-1].start()
    for copy in copies:
        copy.wait()

    def add_half(k, carry):
        value = part[b, k].astype(jnp.float32)
        for d in range(1, B):
            value = value + got1[d - 1, k].astype(jnp.float32)
        half[k] = value.astype(jnp.bfloat16)
        return carry

    lax.fori_loop(0, R, add_half, 0)

    copies = []
    for d in range(1, R):
        to = lax.rem(r + d, R)
        copies.append(
            pltpu.make_async_remote_copy(
                src_ref=half.at[to], dst_ref=got2.at[d - 1], send_sem=s2.at[d], recv_sem=r2.at[d],
                device_id={"row": to}, device_id_type=MESH,
            )
        )
        copies[-1].start()
    for copy in copies:
        copy.wait()
    value = half[r].astype(jnp.float32)
    for d in range(1, R):
        value = value + got2[d - 1].astype(jnp.float32)
    block[...] = value.astype(jnp.bfloat16)

    def to_col(k, d):
        return pltpu.make_async_remote_copy(
            src_ref=block.at[k], dst_ref=got3.at[d - 1], send_sem=s3.at[k], recv_sem=r3.at[d],
            device_id={"col": b * share + k}, device_id_type=MESH,
        )

    for k in range(share):
        for d in range(1, C):
            @pl.when(lax.rem(c + d, C) == b * share + k)
            def _():
                to_col(k, d).start()

    for k in range(share):
        @pl.when(c == b * share + k)
        def _():
            total = block[k].astype(jnp.float32)
            for d in range(1, C):
                to_col(k, d).wait_recv()
                total = total + got3[d - 1].astype(jnp.float32)
            out[...] = total

    def to_pb(d):
        return pltpu.make_async_remote_copy(
            src_ref=out, dst_ref=out, send_sem=s4.at[d], recv_sem=r4.at[0],
            device_id={"pb": lax.rem(b + d, B)}, device_id_type=MESH,
        )

    mine = c // share == b

    @pl.when(mine)
    def _():
        for d in range(1, B):
            to_pb(d).start()
        for d in range(1, B):
            to_pb(d).wait_send()

    @pl.when(jnp.logical_not(mine))
    def _():
        to_pb(1).wait_recv()

    for k in range(share):
        @pl.when(c != b * share + k)
        def _():
            to_col(k, 1).wait_send()


def local(chol, amplitudes):
    B, R, C = lax.axis_size("pb"), lax.axis_size("row"), lax.axis_size("col")
    q_local, rw, cw = chol.shape
    nq = q_local // (R * C)
    n = cw // rw
    occ = amplitudes.shape[0]
    groups = rw // SH
    amp = jnp.pad(amplitudes.reshape(occ, groups, VG), ((0, 0), (0, 0), (OG, 0))).reshape(occ, rw)
    any_spec = pl.BlockSpec(memory_space=pl.ANY)
    vmem_spec = pl.BlockSpec(memory_space=pltpu.VMEM)
    dma = pltpu.SemaphoreType.DMA
    recv, amp_all = pl.pallas_call(
        functools.partial(exchange_kernel, R, C),
        out_shape=(
            jax.ShapeDtypeStruct((R * C, nq, rw, cw), jnp.bfloat16),
            jax.ShapeDtypeStruct((R, occ, rw), jnp.bfloat16),
        ),
        in_specs=[any_spec, any_spec],
        out_specs=(any_spec, any_spec),
        scratch_shapes=[
            pltpu.VMEM((nq, rw, cw), jnp.bfloat16),
            dma((R * C,)),
            dma((R * C,)),
            dma((R,)),
            dma((R,)),
            dma((3,)),
        ],
        compiler_params=pltpu.CompilerParams(collective_id=0, has_side_effects=True),
        name="exchange",
    )(chol, amp)
    if n > 1:
        amp_all = jnp.transpose(amp_all, (1, 0, 2)).reshape(occ, C, cw).transpose(1, 0, 2)
    orbital = lax.broadcasted_iota(jnp.int32, (C, cw, occ), 0) * cw + lax.broadcasted_iota(jnp.int32, (C, cw, occ), 1)
    index = lax.broadcasted_iota(jnp.int32, (C, cw, occ), 2)
    pick = (orbital == index // OG * SH + index % OG).astype(jnp.bfloat16)
    pick_t = jnp.transpose(pick, (0, 2, 1))
    norb = C * cw
    whole = lambda shape: pl.BlockSpec(shape, lambda q: (0,) * len(shape))
    dressed, fock = pl.pallas_call(
        functools.partial(dress_kernel, R, C, n),
        grid=(nq,),
        out_shape=(
            jax.ShapeDtypeStruct((nq, norb, norb), jnp.bfloat16),
            jax.ShapeDtypeStruct((C, C, cw, cw), jnp.bfloat16),
        ),
        in_specs=[
            pl.BlockSpec((R * C, 1, rw, cw), lambda q: (0, q, 0, 0)),
            whole((C, occ, cw)),
            whole((C, cw, occ)),
            whole((C, occ, cw)),
        ],
        out_specs=(
            pl.BlockSpec((1, norb, norb), lambda q: (q, 0, 0)),
            whole((C, C, cw, cw)),
        ),
        scratch_shapes=[
            pltpu.VMEM((C, C, cw, cw), jnp.bfloat16),
            pltpu.VMEM((C, cw, occ), jnp.bfloat16),
            pltpu.VMEM((C, C, cw, cw), jnp.float32),
        ],
        compiler_params=pltpu.CompilerParams(vmem_limit_bytes=60 * 1024 * 1024),
        name="dress",
    )(recv, amp_all, pick, pick_t)
    share = C // B
    part = jnp.transpose(fock.reshape(B, share, R, rw, cw), (0, 2, 1, 3, 4))
    bf16 = lambda *shape: pltpu.VMEM(shape, jnp.bfloat16)
    out = pl.pallas_call(
        functools.partial(reduce_kernel, B, R, C),
        out_shape=jax.ShapeDtypeStruct((rw, cw), jnp.float32),
        in_specs=[vmem_spec],
        out_specs=vmem_spec,
        scratch_shapes=[
            bf16(B - 1, R, share, rw, cw),
            bf16(R, share, rw, cw),
            bf16(R - 1, share, rw, cw),
            bf16(share, rw, cw),
            bf16(C - 1, rw, cw),
            dma((B,)), dma((B,)), dma((R,)), dma((R,)), dma((share,)), dma((C,)), dma((B,)), dma((1,)),
        ],
        compiler_params=pltpu.CompilerParams(
            collective_id=1, has_side_effects=True, vmem_limit_bytes=60 * 1024 * 1024
        ),
        name="reduce",
    )(part)
    return dressed, out


def solution(mesh):
    return jax.shard_map(
        local,
        mesh=mesh,
        in_specs=(P("pb", "row", "col"), P(None, "row")),
        out_specs=(P(("pb", "row", "col"), None, None), P("row", "col")),
        check_vma=False,
    )
```

```python
import functools
import jax
import jax.numpy as jnp
from jax import lax
from jax.experimental import pallas as pl
from jax.experimental.pallas import tpu as pltpu
from jax.sharding import PartitionSpec as P

OG = 9
VG = 75
SH = 84
MESH = pl.DeviceIdType.MESH


def lanes(parts):
    return jnp.concatenate([p.astype(jnp.float32) for p in parts], axis=1).astype(jnp.bfloat16)


def pack(a, b, mid, low, rows):
    first, second = a.astype(jnp.float32), b.astype(jnp.float32)
    wide = jnp.concatenate([first[:, :mid], second[:, :mid]], axis=1).astype(jnp.bfloat16)
    thin = jnp.concatenate([first[:, mid:], second[:, mid:]], axis=0)
    pieces = [thin[k * rows : (k + 1) * rows] for k in range(thin.shape[0] // rows)]
    pieces.append(jnp.zeros((rows, 128 - low * len(pieces)), jnp.float32))
    return wide, jnp.concatenate(pieces, axis=1).astype(jnp.bfloat16)


def unpack(main, wide, thin, which, mid, low, rw):
    wide = wide.astype(jnp.float32)[:, which * mid : (which + 1) * mid]
    thin = thin.astype(jnp.float32)
    rows = thin.shape[0]
    pieces = [thin[:, k * low : (k + 1) * low] for k in range(2 * rw // rows)]
    thin = jnp.concatenate(pieces, axis=0)[which * rw : (which + 1) * rw]
    return jnp.concatenate([main.astype(jnp.float32), wide, thin], axis=1)


def dress(R, C, n, which, mid, low, mains, wides, thins, amps, pick, pick_t, primed, cols, put_dressed, put_fock):
    rw = mains.shape[1]
    th = rw * n
    for j in range(C):
        shift = None
        for i in range(C):
            pieces = []
            for m in range(n):
                s = (i * n + m) * C + j
                pieces.append(unpack(mains[s], wides[s], thins[s], which, mid, low, rw))
            tile = (pieces[0] if n == 1 else jnp.concatenate(pieces, axis=0)).astype(jnp.bfloat16)
            primed[i, j] = tile
            term = jnp.dot(amps[i], tile, preferred_element_type=jnp.float32)
            term = term.astype(jnp.bfloat16).astype(jnp.float32)
            shift = term if shift is None else shift + term
        hi = shift.astype(jnp.bfloat16)
        lo = (shift - hi.astype(jnp.float32)).astype(jnp.bfloat16)
        for i in range(C):
            placed = jnp.dot(pick[i], hi, preferred_element_type=jnp.float32)
            placed = placed + jnp.dot(pick[i], lo, preferred_element_type=jnp.float32)
            primed[i, j] = (primed[i, j].astype(jnp.float32) - placed).astype(jnp.bfloat16)
    weight = jnp.zeros((1, 1), jnp.float32)
    for i in range(C):
        occ = None
        for j in range(C):
            part = jnp.dot(primed[i, j], pick[j], preferred_element_type=jnp.float32)
            occ = part if occ is None else occ + part
        cols[i] = occ.astype(jnp.bfloat16)
        diag = occ * pick[i].astype(jnp.float32)
        weight = weight + jnp.sum(jnp.sum(diag, axis=1, keepdims=True), axis=0, keepdims=True)
    for i in range(C):
        strip = []
        for j in range(C):
            extra = jnp.dot(cols[i], amps[j], preferred_element_type=jnp.float32)
            tile = (primed[i, j].astype(jnp.float32) + extra).astype(jnp.bfloat16)
            primed[i, j] = tile
            strip.append(tile)
        put_dressed(i, lanes(strip))
    for j in range(C):
        rows = None
        for i in range(C):
            part = jnp.dot(pick_t[i], primed[i, j], preferred_element_type=jnp.float32)
            rows = part if rows is None else rows + part
        rows = rows.astype(jnp.bfloat16)
        for i in range(C):
            swapped = jnp.dot(cols[i], rows, preferred_element_type=jnp.float32)
            put_fock(i, j, 2.0 * weight * primed[i, j].astype(jnp.float32) - swapped)


def exchange_kernel(
    R, C, n, mid, low, rows, chol, amp, pick, pick_t,
    main_b, wide_all, thin_all, amps, dressed, fock,
    tails, wide_out, thin_out, own, amp_all, mains, wides, thins, primed, cols,
    send, recv, lsem,
):
    r = lax.axis_index("row")
    c = lax.axis_index("col")
    me = r * C + c
    rw = chol.shape[1]
    full = mains.shape[2]
    tail_in = pltpu.make_async_copy(chol.at[:, :, pl.ds(full, mid + low)], tails, lsem.at[0])
    tail_in.start()
    own_in = pltpu.make_async_copy(chol.at[pl.ds(me * 2, 2), :, pl.ds(0, full)], own, lsem.at[1])
    own_in.start()
    amp_in = pltpu.make_async_copy(amp, amp_all.at[r], lsem.at[2])
    amp_in.start()
    peers = [(dr, dc) for dr in range(R) for dc in range(C) if (dr, dc) != (0, 0)]
    peers.sort(key=lambda t: -min(t[1], C - t[1]))
    barrier = pltpu.get_barrier_semaphore()
    for dr, dc in peers:
        pl.semaphore_signal(
            barrier, inc=1, device_id={"row": lax.rem(r + dr, R), "col": lax.rem(c + dc, C)}, device_id_type=MESH
        )
    pl.semaphore_wait(barrier, len(peers))

    def move(kind, src, dst, dr, dc):
        return pltpu.make_async_remote_copy(
            src_ref=src,
            dst_ref=dst,
            send_sem=send.at[kind, dr * C + dc],
            recv_sem=recv.at[kind, dr * C + dc],
            device_id={"row": lax.rem(r + dr, R), "col": lax.rem(c + dc, C)},
            device_id_type=MESH,
        )

    amp_moves = [move(0, amp, amp_all.at[r], dr, 0) for dr in range(1, R)]
    for copy in amp_moves:
        copy.start()
    first, second = [], []
    for dr, dc in peers:
        to = lax.rem(r + dr, R) * C + lax.rem(c + dc, C)
        first.append(move(1, chol.at[to * 2, :, pl.ds(0, full)], mains.at[me], dr, dc))
        first[-1].start()
    tail_in.wait()

    def pack_one(d, carry):
        wide, thin = pack(tails[2 * d], tails[2 * d + 1], mid, low, rows)
        wide_out[d] = wide
        thin_out[d] = thin
        return carry

    lax.fori_loop(0, R * C, pack_one, 0)
    for dr, dc in peers:
        to = lax.rem(r + dr, R) * C + lax.rem(c + dc, C)
        first.append(move(2, wide_out.at[to], wide_all.at[me], dr, dc))
        first.append(move(3, thin_out.at[to], thin_all.at[me], dr, dc))
        first[-2].start()
        first[-1].start()
    for dr, dc in peers:
        to = lax.rem(r + dr, R) * C + lax.rem(c + dc, C)
        second.append(move(4, chol.at[to * 2 + 1, :, pl.ds(0, full)], main_b.at[me], dr, dc))
        second[-1].start()
    own_in.wait()
    amp_in.wait()
    mains[me] = own[0]
    local = [
        pltpu.make_async_copy(own.at[1], main_b.at[me], lsem.at[3]),
        pltpu.make_async_copy(wide_out.at[me], wide_all.at[me], lsem.at[4]),
        pltpu.make_async_copy(thin_out.at[me], thin_all.at[me], lsem.at[5]),
    ]
    for copy in local:
        copy.start()
    for copy in amp_moves:
        copy.wait()
    for i in range(C):
        amps[i] = amp_all[i] if n == 1 else lanes([amp_all[i * n + m] for m in range(n)])
    for copy in local:
        copy.wait()
    for copy in first:
        copy.wait()
    loads = [
        pltpu.make_async_copy(wide_all, wides, lsem.at[6]),
        pltpu.make_async_copy(thin_all, thins, lsem.at[7]),
    ]
    for copy in loads:
        copy.start()
    for copy in loads:
        copy.wait()
    th = rw * n

    def put_dressed(i, strip):
        dressed[0, pl.ds(i * th, th), :] = strip

    def put_fock(i, j, value):
        fock[i, j] = value

    dress(R, C, n, 0, mid, low, mains, wides, thins, amps, pick, pick_t, primed, cols, put_dressed, put_fock)
    for copy in second:
        copy.wait()


def dress_kernel(
    R, C, n, B, mid, low, mains, wides, thins, amps, pick, pick_t, before, before_fock,
    dressed, fock, primed, cols, held, result, partial, sem,
):
    share = C // B
    th = mains.shape[1] * n
    load = pltpu.make_async_copy(before, held, sem.at[0])
    load.start()
    load_fock = pltpu.make_async_copy(before_fock, partial, sem.at[1])
    load_fock.start()
    store = pltpu.make_async_copy(held, dressed.at[pl.ds(0, 1)], sem.at[2])
    final = pltpu.make_async_copy(result, dressed.at[pl.ds(1, 1)], sem.at[3])

    def put_dressed(i, strip):
        if i == 0:
            load.wait()
            store.start()
        result[0, pl.ds(i * th, th), :] = strip
        if i == C - 1:
            load_fock.wait()
            final.start()

    def put_fock(i, j, value):
        fock[j // share, i, j % share] = (partial[i, j] + value).astype(jnp.bfloat16)

    dress(R, C, n, 1, mid, low, mains, wides, thins, amps, pick, pick_t, primed, cols, put_dressed, put_fock)
    store.wait()
    final.wait()


def reduce_kernel(B, R, C, part, out, got1, half, got2, block, got3, s1, r1, s2, r2, s3, r3, s4, r4):
    b = lax.axis_index("pb")
    r = lax.axis_index("row")
    c = lax.axis_index("col")
    share = C // B
    barrier = pltpu.get_barrier_semaphore()
    for axis, index, size in (("pb", b, B), ("row", r, R), ("col", c, C)):
        for d in range(1, size):
            pl.semaphore_signal(barrier, inc=1, device_id={axis: lax.rem(index + d, size)}, device_id_type=MESH)
    pl.semaphore_wait(barrier, B + R + C - 3)
    order = list(range(1, R)) + [0]

    def to_half(k, d, e):
        to, row = lax.rem(b + e, B), lax.rem(r + d, R)
        return pltpu.make_async_remote_copy(
            src_ref=part.at[to, row, k], dst_ref=got1.at[e - 1, k, d],
            send_sem=s1.at[e, k, d], recv_sem=r1.at[e, k, d],
            device_id={"pb": to}, device_id_type=MESH,
        )

    def to_row(k, d):
        return pltpu.make_async_remote_copy(
            src_ref=half.at[k, d], dst_ref=got2.at[k, d], send_sem=s2.at[k, d], recv_sem=r2.at[k, d],
            device_id={"row": lax.rem(r + d, R)}, device_id_type=MESH,
        )

    def to_col(k, d):
        return pltpu.make_async_remote_copy(
            src_ref=block.at[k], dst_ref=got3.at[d - 1], send_sem=s3.at[k], recv_sem=r3.at[d],
            device_id={"col": b * share + k}, device_id_type=MESH,
        )

    for k in range(share):
        for d in order:
            for e in range(1, B):
                to_half(k, d, e).start()
    for k in range(share):
        for d in order:
            value = part[b, lax.rem(r + d, R), k].astype(jnp.float32)
            for e in range(1, B):
                to_half(k, d, e).wait()
                value = value + got1[e - 1, k, d].astype(jnp.float32)
            half[k, d] = value.astype(jnp.bfloat16)
            if d:
                to_row(k, d).start()
    for k in range(share):
        value = half[k, 0].astype(jnp.float32)
        for d in range(1, R):
            to_row(k, d).wait()
            value = value + got2[k, d].astype(jnp.float32)
        block[k] = value.astype(jnp.bfloat16)
        for d in range(1, C):
            @pl.when(lax.rem(c + d, C) == b * share + k)
            def _():
                to_col(k, d).start()

    for k in range(share):
        @pl.when(c == b * share + k)
        def _():
            total = block[k].astype(jnp.float32)
            for d in range(1, C):
                to_col(k, d).wait_recv()
                total = total + got3[d - 1].astype(jnp.float32)
            out[...] = total

    def to_pb(d):
        return pltpu.make_async_remote_copy(
            src_ref=out, dst_ref=out, send_sem=s4.at[d], recv_sem=r4.at[0],
            device_id={"pb": lax.rem(b + d, B)}, device_id_type=MESH,
        )

    mine = c // share == b

    @pl.when(mine)
    def _():
        for d in range(1, B):
            to_pb(d).start()
        for d in range(1, B):
            to_pb(d).wait_send()

    @pl.when(jnp.logical_not(mine))
    def _():
        to_pb(1).wait_recv()

    for k in range(share):
        @pl.when(c != b * share + k)
        def _():
            to_col(k, 1).wait_send()


def local(chol, amplitudes):
    B, R, C = lax.axis_size("pb"), lax.axis_size("row"), lax.axis_size("col")
    q_local, rw, cw = chol.shape
    n = cw // rw
    norb = C * cw
    occ = amplitudes.shape[0]
    groups = rw // SH
    full = cw // 128 * 128
    mid = 64
    low = cw - full - mid
    rows = 2 * rw // 7
    share = C // B
    amp = jnp.pad(amplitudes.reshape(occ, groups, VG), ((0, 0), (0, 0), (OG, 0))).reshape(occ, rw)
    orbital = lax.broadcasted_iota(jnp.int32, (C, cw, occ), 0) * cw + lax.broadcasted_iota(jnp.int32, (C, cw, occ), 1)
    index = lax.broadcasted_iota(jnp.int32, (C, cw, occ), 2)
    pick = (orbital == index // OG * SH + index % OG).astype(jnp.bfloat16)
    pick_t = jnp.transpose(pick, (0, 2, 1))
    hbm = pl.BlockSpec(memory_space=pl.ANY)
    vmem = pl.BlockSpec(memory_space=pltpu.VMEM)
    dma = pltpu.SemaphoreType.DMA
    bf16 = lambda *shape: pltpu.VMEM(shape, jnp.bfloat16)
    shape = lambda *dims: jax.ShapeDtypeStruct(dims, jnp.bfloat16)
    limit = 60 * 1024 * 1024
    N = R * C
    main_b, wide_all, thin_all, amps, before, before_fock = pl.pallas_call(
        functools.partial(exchange_kernel, R, C, n, mid, low, rows),
        out_shape=(
            shape(N, rw, full),
            shape(N, rw, 128),
            shape(N, rows, 128),
            shape(C, occ, cw),
            shape(1, norb, norb),
            jax.ShapeDtypeStruct((C, C, cw, cw), jnp.float32),
        ),
        in_specs=[hbm, hbm, vmem, vmem],
        out_specs=(hbm, hbm, hbm, vmem, vmem, vmem),
        scratch_shapes=[
            bf16(q_local, rw, mid + low),
            bf16(N, rw, 128),
            bf16(N, rows, 128),
            bf16(2, rw, full),
            bf16(R, occ, rw),
            bf16(N, rw, full),
            bf16(N, rw, 128),
            bf16(N, rows, 128),
            bf16(C, C, cw, cw),
            bf16(C, cw, occ),
            dma((5, N)),
            dma((5, N)),
            dma((8,)),
        ],
        compiler_params=pltpu.CompilerParams(collective_id=0, has_side_effects=True, vmem_limit_bytes=limit),
        name="exchange",
    )(chol, amp, pick, pick_t)
    dressed, fock = pl.pallas_call(
        functools.partial(dress_kernel, R, C, n, B, mid, low),
        out_shape=(shape(2, norb, norb), shape(B, C, share, cw, cw)),
        in_specs=[vmem] * 6 + [hbm, hbm],
        out_specs=(hbm, vmem),
        scratch_shapes=[
            bf16(C, C, cw, cw),
            bf16(C, cw, occ),
            bf16(1, norb, norb),
            bf16(1, norb, norb),
            pltpu.VMEM((C, C, cw, cw), jnp.float32),
            dma((4,)),
        ],
        compiler_params=pltpu.CompilerParams(vmem_limit_bytes=limit),
        name="dress",
    )(main_b, wide_all, thin_all, amps, pick, pick_t, before, before_fock)
    part = fock
    if n > 1:
        part = jnp.transpose(fock.reshape(B, C, share, n, rw, cw), (0, 1, 3, 2, 4, 5)).reshape(B, R, share, rw, cw)
    out = pl.pallas_call(
        functools.partial(reduce_kernel, B, R, C),
        out_shape=jax.ShapeDtypeStruct((rw, cw), jnp.float32),
        in_specs=[vmem],
        out_specs=vmem,
        scratch_shapes=[
            bf16(B - 1, share, R, rw, cw),
            bf16(share, R, rw, cw),
            bf16(share, R, rw, cw),
            bf16(share, rw, cw),
            bf16(C - 1, rw, cw),
            dma((B, share, R)), dma((B, share, R)), dma((share, R)), dma((share, R)),
            dma((share,)), dma((C,)), dma((B,)), dma((1,)),
        ],
        compiler_params=pltpu.CompilerParams(collective_id=1, has_side_effects=True, vmem_limit_bytes=limit),
        name="reduce",
    )(part)
    return dressed, out


def solution(mesh):
    return jax.shard_map(
        local,
        mesh=mesh,
        in_specs=(P("pb", "row", "col"), P(None, "row")),
        out_specs=(P(("pb", "row", "col"), None, None), P("row", "col")),
        check_vma=False,
    )
```

```python
import functools
import jax
import numpy as np
import jax.numpy as jnp
from jax import lax
from jax.experimental import pallas as pl
from jax.experimental.pallas import tpu as pltpu
from jax.sharding import PartitionSpec as P

OG = 9
VG = 75
SH = 84
MESH = pl.DeviceIdType.MESH


def peer(index, mode, size):
    if size & (size - 1):
        return lax.rem(index + mode, size)
    bits = [1 << k for k in range(size.bit_length() - 1)]
    return sum(lax.rem(lax.rem(lax.div(index, bit), 2) + mode // bit % 2, 2) * bit for bit in bits)


def lanes(parts):
    return jnp.concatenate([p.astype(jnp.float32) for p in parts], axis=1).astype(jnp.bfloat16)


def pack(a, b, mid, low, rows):
    first, second = a.astype(jnp.float32), b.astype(jnp.float32)
    wide = jnp.concatenate([first[:, :mid], second[:, :mid]], axis=1).astype(jnp.bfloat16)
    thin = jnp.concatenate([first[:, mid:], second[:, mid:]], axis=0)
    pieces = [thin[k * rows : (k + 1) * rows] for k in range(thin.shape[0] // rows)]
    pieces.append(jnp.zeros((rows, 128 - low * len(pieces)), jnp.float32))
    return wide, jnp.concatenate(pieces, axis=1).astype(jnp.bfloat16)


def unpack_tail(wide, thin, which, mid, low, rw):
    wide = wide.astype(jnp.float32)[:, which * mid : (which + 1) * mid]
    thin = thin.astype(jnp.float32)
    rows = thin.shape[0]
    pieces = [thin[:, k * low : (k + 1) * low] for k in range(2 * rw // rows)]
    thin = jnp.concatenate(pieces, axis=0)[which * rw : (which + 1) * rw]
    return jnp.concatenate([wide, thin], axis=1)


def dress(R, C, n, mains, tail, amps, pick, pick_t, primed, cols, put_dressed, put_fock):
    rw = mains.shape[1]
    th = rw * n
    for j in range(C):
        shift = None
        for i in range(C):
            pieces = []
            for m in range(n):
                s = (i * n + m) * C + j
                pieces.append(jnp.concatenate([mains[s], tail[s]], axis=1))
            tile = pieces[0]
            if n > 1:
                tile = jnp.concatenate([p.astype(jnp.float32) for p in pieces], axis=0).astype(jnp.bfloat16)
            primed[i, j] = tile
            term = jnp.dot(amps[i], tile, preferred_element_type=jnp.float32)
            term = term.astype(jnp.bfloat16).astype(jnp.float32)
            shift = term if shift is None else shift + term
        hi = shift.astype(jnp.bfloat16)
        lo = (shift - hi.astype(jnp.float32)).astype(jnp.bfloat16)
        for i in range(C):
            placed = jnp.dot(pick[i], hi, preferred_element_type=jnp.float32)
            placed = placed + jnp.dot(pick[i], lo, preferred_element_type=jnp.float32)
            primed[i, j] = (primed[i, j].astype(jnp.float32) - placed).astype(jnp.bfloat16)
    weight = jnp.zeros((1, 1), jnp.float32)
    for i in range(C):
        occ = None
        for j in range(C):
            part = jnp.dot(primed[i, j], pick[j], preferred_element_type=jnp.float32)
            occ = part if occ is None else occ + part
        cols[i] = occ.astype(jnp.bfloat16)
        diag = occ * pick[i].astype(jnp.float32)
        weight = weight + jnp.sum(jnp.sum(diag, axis=1, keepdims=True), axis=0, keepdims=True)
    for i in range(C):
        strip = []
        for j in range(C):
            extra = jnp.dot(cols[i], amps[j], preferred_element_type=jnp.float32)
            tile = (primed[i, j].astype(jnp.float32) + extra).astype(jnp.bfloat16)
            primed[i, j] = tile
            strip.append(tile)
        put_dressed(i, lanes(strip))
    for j in range(C):
        rows = None
        for i in range(C):
            part = jnp.dot(pick_t[i], primed[i, j], preferred_element_type=jnp.float32)
            rows = part if rows is None else rows + part
        rows = rows.astype(jnp.bfloat16)
        for i in range(C):
            swapped = jnp.dot(cols[i], rows, preferred_element_type=jnp.float32)
            put_fock(i, j, 2.0 * weight * primed[i, j].astype(jnp.float32) - swapped)


def exchange_kernel(
    R, C, n, mid, low, rows, chol, amp, widen, pick, pick_t,
    main_b, wide_all, thin_all, tail_b, amps, dressed, fock,
    tails, wide_out, thin_out, own, amp_out, amp_all, mains, tail_a, wides, thins, primed, cols,
    send, recv, lsem,
):
    r = lax.axis_index("row")
    c = lax.axis_index("col")
    me = r * C + c
    rw = chol.shape[1]
    full = mains.shape[2]
    tail_in = pltpu.make_async_copy(chol.at[:, :, pl.ds(full, mid + low)], tails, lsem.at[0])
    tail_in.start()
    own_in = pltpu.make_async_copy(chol.at[pl.ds(me * 2, 2), :, pl.ds(0, full)], own, lsem.at[1])
    own_in.start()
    peers = [(dr, dc) for dr in range(R) for dc in range(C) if (dr, dc) != (0, 0)]
    peers.sort(key=lambda t: -t[1].bit_length())
    barrier = pltpu.get_barrier_semaphore()
    for dr, dc in peers:
        pl.semaphore_signal(
            barrier, inc=1, device_id={"row": peer(r, dr, R), "col": peer(c, dc, C)}, device_id_type=MESH
        )
    wide_amp = jnp.dot(amp[...], widen[...], preferred_element_type=jnp.float32).astype(jnp.bfloat16)
    amp_out[...] = wide_amp
    pl.semaphore_wait(barrier, len(peers))

    def move(kind, src, dst, dr, dc):
        return pltpu.make_async_remote_copy(
            src_ref=src,
            dst_ref=dst,
            send_sem=send.at[kind, dr * C + dc],
            recv_sem=recv.at[kind, dr * C + dc],
            device_id={"row": peer(r, dr, R), "col": peer(c, dc, C)},
            device_id_type=MESH,
        )

    first, second = [], []
    for dr, dc in peers:
        to = peer(r, dr, R) * C + peer(c, dc, C)
        first.append(move(1, chol.at[to * 2, :, pl.ds(0, full)], mains.at[me], dr, dc))
        first[-1].start()
    amp_moves = [move(0, amp_out, amp_all.at[r], dr, 0) for dr in range(1, R)]
    for copy in amp_moves:
        copy.start()
    amp_all[r] = wide_amp
    tail_in.wait()

    def pack_one(d, carry):
        wide, thin = pack(tails[2 * d], tails[2 * d + 1], mid, low, rows)
        wide_out[d] = wide
        thin_out[d] = thin
        return carry

    lax.fori_loop(0, R * C, pack_one, 0)
    for dr, dc in peers:
        to = peer(r, dr, R) * C + peer(c, dc, C)
        first.append(move(2, wide_out.at[to], wide_all.at[me], dr, dc))
        first.append(move(3, thin_out.at[to], thin_all.at[me], dr, dc))
        first[-2].start()
        first[-1].start()
    for dr, dc in peers:
        to = peer(r, dr, R) * C + peer(c, dc, C)
        second.append(move(4, chol.at[to * 2 + 1, :, pl.ds(0, full)], main_b.at[me], dr, dc))
        second[-1].start()
    own_in.wait()
    mains[me] = own[0]
    local = [
        pltpu.make_async_copy(own.at[1], main_b.at[me], lsem.at[3]),
        pltpu.make_async_copy(wide_out.at[me], wide_all.at[me], lsem.at[4]),
        pltpu.make_async_copy(thin_out.at[me], thin_all.at[me], lsem.at[5]),
    ]
    for copy in local:
        copy.start()
    for copy in amp_moves:
        copy.wait()
    for i in range(C):
        amps[i] = amp_all[i] if n == 1 else lanes([amp_all[i * n + m] for m in range(n)])
    for copy in local:
        copy.wait()
    for copy in first:
        copy.wait()
    loads = [
        pltpu.make_async_copy(wide_all, wides, lsem.at[6]),
        pltpu.make_async_copy(thin_all, thins, lsem.at[7]),
    ]
    for copy in loads:
        copy.start()
    for copy in loads:
        copy.wait()
    th = rw * n

    def open_tail(s, carry):
        tail_a[s] = unpack_tail(wides[s], thins[s], 0, mid, low, rw).astype(jnp.bfloat16)
        tail_b[s] = unpack_tail(wides[s], thins[s], 1, mid, low, rw).astype(jnp.bfloat16)
        return carry

    lax.fori_loop(0, R * C, open_tail, 0)

    def put_dressed(i, strip):
        dressed[0, pl.ds(i * th, th), :] = strip

    def put_fock(i, j, value):
        fock[i, j] = value

    dress(R, C, n, mains, tail_a, amps, pick, pick_t, primed, cols, put_dressed, put_fock)
    for copy in second:
        copy.wait()


def dress_kernel(
    R, C, n, B, mains, tail, amps, pick, pick_t, before, before_fock,
    dressed, fock, primed, cols, held, result, partial, sem,
):
    share = C // B
    th = mains.shape[1] * n
    load = pltpu.make_async_copy(before, held, sem.at[0])
    load.start()
    load_fock = pltpu.make_async_copy(before_fock, partial, sem.at[1])
    load_fock.start()
    store = pltpu.make_async_copy(held, dressed.at[pl.ds(0, 1)], sem.at[2])
    final = pltpu.make_async_copy(result, dressed.at[pl.ds(1, 1)], sem.at[3])

    def put_dressed(i, strip):
        if i == 0:
            load.wait()
            store.start()
        result[0, pl.ds(i * th, th), :] = strip
        if i == C - 1:
            load_fock.wait()
            final.start()

    def put_fock(i, j, value):
        fock[j // share, i, j % share] = (partial[i, j] + value).astype(jnp.bfloat16)

    dress(R, C, n, mains, tail, amps, pick, pick_t, primed, cols, put_dressed, put_fock)
    store.wait()
    final.wait()


def reduce_kernel(B, R, C, part, out, got1, half, got2, block, got3, s1, r1, s2, r2, s3, r3, s4, r4):
    b = lax.axis_index("pb")
    r = lax.axis_index("row")
    c = lax.axis_index("col")
    share = C // B
    barrier = pltpu.get_barrier_semaphore()
    for axis, index, size in (("pb", b, B), ("row", r, R), ("col", c, C)):
        for d in range(1, size):
            pl.semaphore_signal(barrier, inc=1, device_id={axis: lax.rem(index + d, size)}, device_id_type=MESH)
    pl.semaphore_wait(barrier, B + R + C - 3)
    order = list(range(1, R)) + [0]

    def to_half(k, d, e):
        to, row = lax.rem(b + e, B), lax.rem(r + d, R)
        return pltpu.make_async_remote_copy(
            src_ref=part.at[to, row, k], dst_ref=got1.at[e - 1, k, d],
            send_sem=s1.at[e, k, d], recv_sem=r1.at[e, k, d],
            device_id={"pb": to}, device_id_type=MESH,
        )

    def to_row(k, d):
        return pltpu.make_async_remote_copy(
            src_ref=half.at[k, d], dst_ref=got2.at[k, d], send_sem=s2.at[k, d], recv_sem=r2.at[k, d],
            device_id={"row": lax.rem(r + d, R)}, device_id_type=MESH,
        )

    def to_col(k, d):
        return pltpu.make_async_remote_copy(
            src_ref=block.at[k], dst_ref=got3.at[d - 1], send_sem=s3.at[k], recv_sem=r3.at[d],
            device_id={"col": b * share + k}, device_id_type=MESH,
        )

    for k in range(share):
        for d in order:
            for e in range(1, B):
                to_half(k, d, e).start()
    for k in range(share):
        for d in order:
            value = part[b, lax.rem(r + d, R), k].astype(jnp.float32)
            for e in range(1, B):
                to_half(k, d, e).wait()
                value = value + got1[e - 1, k, d].astype(jnp.float32)
            half[k, d] = value.astype(jnp.bfloat16)
            if d:
                to_row(k, d).start()
    for k in range(share):
        value = half[k, 0].astype(jnp.float32)
        for d in range(1, R):
            to_row(k, d).wait()
            value = value + got2[k, d].astype(jnp.float32)
        block[k] = value.astype(jnp.bfloat16)
        for d in range(1, C):
            @pl.when(lax.rem(c + d, C) == b * share + k)
            def _():
                to_col(k, d).start()

    for k in range(share):
        @pl.when(c == b * share + k)
        def _():
            total = block[k].astype(jnp.float32)
            for d in range(1, C):
                to_col(k, d).wait_recv()
                total = total + got3[d - 1].astype(jnp.float32)
            out[...] = total

    def to_pb(d):
        return pltpu.make_async_remote_copy(
            src_ref=out, dst_ref=out, send_sem=s4.at[d], recv_sem=r4.at[0],
            device_id={"pb": lax.rem(b + d, B)}, device_id_type=MESH,
        )

    mine = c // share == b

    @pl.when(mine)
    def _():
        for d in range(1, B):
            to_pb(d).start()
        for d in range(1, B):
            to_pb(d).wait_send()

    @pl.when(jnp.logical_not(mine))
    def _():
        to_pb(1).wait_recv()

    for k in range(share):
        @pl.when(c != b * share + k)
        def _():
            to_col(k, 1).wait_send()


def local(chol, amplitudes):
    B, R, C = lax.axis_size("pb"), lax.axis_size("row"), lax.axis_size("col")
    q_local, rw, cw = chol.shape
    n = cw // rw
    norb = C * cw
    occ = amplitudes.shape[0]
    groups = rw // SH
    full = cw // 128 * 128
    mid = 64
    low = cw - full - mid
    rows = 2 * rw // 7
    share = C // B
    virtual = np.arange(groups * VG)
    widen = virtual[:, None] // VG * SH + OG + virtual[:, None] % VG == np.arange(rw)[None, :]
    widen = jnp.asarray(widen, jnp.bfloat16)
    index = np.arange(occ)
    place = np.arange(norb)[:, None] == (index // OG * SH + index % OG)[None, :]
    place = place.reshape(C, cw, occ)
    pick = jnp.asarray(place, jnp.bfloat16)
    pick_t = jnp.asarray(place.transpose(0, 2, 1), jnp.bfloat16)
    hbm = pl.BlockSpec(memory_space=pl.ANY)
    vmem = pl.BlockSpec(memory_space=pltpu.VMEM)
    dma = pltpu.SemaphoreType.DMA
    bf16 = lambda *shape: pltpu.VMEM(shape, jnp.bfloat16)
    shape = lambda *dims: jax.ShapeDtypeStruct(dims, jnp.bfloat16)
    limit = 60 * 1024 * 1024
    N = R * C
    main_b, wide_all, thin_all, tail_b, amps, before, before_fock = pl.pallas_call(
        functools.partial(exchange_kernel, R, C, n, mid, low, rows),
        out_shape=(
            shape(N, rw, full),
            shape(N, rw, 128),
            shape(N, rows, 128),
            shape(N, rw, mid + low),
            shape(C, occ, cw),
            shape(1, norb, norb),
            jax.ShapeDtypeStruct((C, C, cw, cw), jnp.float32),
        ),
        in_specs=[hbm, vmem, vmem, vmem, vmem],
        out_specs=(hbm, hbm, hbm, vmem, vmem, vmem, vmem),
        scratch_shapes=[
            bf16(q_local, rw, mid + low),
            bf16(N, rw, 128),
            bf16(N, rows, 128),
            bf16(2, rw, full),
            bf16(occ, rw),
            bf16(R, occ, rw),
            bf16(N, rw, full),
            bf16(N, rw, mid + low),
            bf16(N, rw, 128),
            bf16(N, rows, 128),
            bf16(C, C, cw, cw),
            bf16(C, cw, occ),
            dma((5, N)),
            dma((5, N)),
            dma((8,)),
        ],
        compiler_params=pltpu.CompilerParams(collective_id=0, has_side_effects=True, vmem_limit_bytes=limit),
        name="exchange",
    )(chol, amplitudes, widen, pick, pick_t)
    dressed, fock = pl.pallas_call(
        functools.partial(dress_kernel, R, C, n, B),
        out_shape=(shape(2, norb, norb), shape(B, C, share, cw, cw)),
        in_specs=[vmem] * 5 + [hbm, hbm],
        out_specs=(hbm, vmem),
        scratch_shapes=[
            bf16(C, C, cw, cw),
            bf16(C, cw, occ),
            bf16(1, norb, norb),
            bf16(1, norb, norb),
            pltpu.VMEM((C, C, cw, cw), jnp.float32),
            dma((4,)),
        ],
        compiler_params=pltpu.CompilerParams(vmem_limit_bytes=limit),
        name="dress",
    )(main_b, tail_b, amps, pick, pick_t, before, before_fock)
    part = fock
    if n > 1:
        part = jnp.transpose(fock.reshape(B, C, share, n, rw, cw), (0, 1, 3, 2, 4, 5)).reshape(B, R, share, rw, cw)
    out = pl.pallas_call(
        functools.partial(reduce_kernel, B, R, C),
        out_shape=jax.ShapeDtypeStruct((rw, cw), jnp.float32),
        in_specs=[vmem],
        out_specs=vmem,
        scratch_shapes=[
            bf16(B - 1, share, R, rw, cw),
            bf16(share, R, rw, cw),
            bf16(share, R, rw, cw),
            bf16(share, rw, cw),
            bf16(C - 1, rw, cw),
            dma((B, share, R)), dma((B, share, R)), dma((share, R)), dma((share, R)),
            dma((share,)), dma((C,)), dma((B,)), dma((1,)),
        ],
        compiler_params=pltpu.CompilerParams(collective_id=1, has_side_effects=True, vmem_limit_bytes=limit),
        name="reduce",
    )(part)
    return dressed, out


def solution(mesh):
    return jax.shard_map(
        local,
        mesh=mesh,
        in_specs=(P("pb", "row", "col"), P(None, "row")),
        out_specs=(P(("pb", "row", "col"), None, None), P("row", "col")),
        check_vma=False,
    )
```
